8 devices in a mesh: dp: 2 (over z, y), tp: 4 (over x, core).
Axes of the slice: x: 2, y: 2, z: 1, core: 2. Of those that a mesh axis runs over, the one named last changes fastest.
Arguments:
- x_in: bfloat16 [128, 128, 4096], P('dp'), parts along dimension 0
- adapter_ids: int32 [128], P('dp'), parts along dimension 0
- gain_attn: float32 [4096], replicated
- gain_mlp: float32 [4096], replicated
- w_q: bfloat16 [4096, 32, 128], P(None, 'tp')
- w_k: bfloat16 [4096, 32, 128], P(None, 'tp')
- w_v: bfloat16 [4096, 32, 128], P(None, 'tp')
- w_o: bfloat16 [32, 128, 4096], P('tp')
- w_gate: bfloat16 [4096, 11008], P(None, 'tp')
- w_up: bfloat16 [4096, 11008], P(None, 'tp')
- w_down: bfloat16 [11008, 4096], P('tp')
- a_q: bfloat16 [8, 4096, 16], P(None, None, 'tp')
- b_q: bfloat16 [8, 16, 32, 128], P(None, None, 'tp')
- a_k: bfloat16 [8, 4096, 16], P(None, None, 'tp')
- b_k: bfloat16 [8, 16, 32, 128], P(None, None, 'tp')
- a_v: bfloat16 [8, 4096, 16], P(None, None, 'tp')
- b_v: bfloat16 [8, 16, 32, 128], P(None, None, 'tp')
- a_o: bfloat16 [8, 32, 128, 16], P(None, 'tp')
- b_o: bfloat16 [8, 16, 4096], P(None, None, 'tp')
- a_gate: bfloat16 [8, 4096, 16], P(None, None, 'tp')
- b_gate: bfloat16 [8, 16, 11008], P(None, None, 'tp')
- a_up: bfloat16 [8, 4096, 16], P(None, None, 'tp')
- b_up: bfloat16 [8, 16, 11008], P(None, None, 'tp')
- a_down: bfloat16 [8, 11008, 16], P(None, 'tp')
- b_down: bfloat16 [8, 16, 4096], P(None, None, 'tp')
Outputs:
- output: bfloat16 [128, 128, 4096], P('dp'), parts along dimension 0
There are 2 independent parts. The reference program is written for one: setup_inputs(seed, part) draws one part's arguments, and reference() takes and returns one part's arrays. A program takes and returns all parts, laid end to end along the dimension named above; an argument that names none is the same for every part.
All inputs are finite; a program needn't handle non-finite values.
Results may differ from the reference program's by a relative error of at most 0.02.
Values are sent between devices in bfloat16 or wider.
A program may use at most 1 GiB of HBM per device.

```python
import jax
import jax.numpy as jnp
from jax import lax

BATCH = 64
SEQ_LEN = 128
D_MODEL = 4096
HEADS = 32
KV_HEADS = 32
HEAD_DIM = 128
D_FF = 11008
RANK = 16
ADAPTERS = 8
LORA_ALPHA = 16
RMS_EPS = 1e-5
Q_WIDTH = HEADS * HEAD_DIM
KV_WIDTH = KV_HEADS * HEAD_DIM


def draw_normal(rng_key, arr_shape, w_std):
    return (jax.random.normal(rng_key, arr_shape, jnp.float32) * w_std).astype(jnp.bfloat16)


def lora_pair(rng_key, a_shape, b_shape, fan_in, w_gain):
    key_a, key_b = jax.random.split(rng_key)
    a_stack = draw_normal(key_a, a_shape, fan_in ** -0.5)
    b_stack = draw_normal(key_b, b_shape, 0.2 * w_gain * RANK ** 0.5 / LORA_ALPHA)
    return a_stack, b_stack


def draw_ids(rng_key):
    key_perm, key_fill, key_mix = jax.random.split(rng_key, 3)
    id_perm = jax.random.permutation(key_perm, ADAPTERS).astype(jnp.int32)
    id_fill = jax.random.randint(key_fill, (BATCH,), 0, ADAPTERS).astype(jnp.int32)
    id_all = jnp.concatenate([id_perm, id_fill])[:BATCH]
    return jax.random.permutation(key_mix, id_all).astype(jnp.int32)


def setup_inputs(seed: int = 0, part: int = 0) -> dict:
    root_key = jax.random.key(seed)
    key_x, key_ids = jax.random.split(jax.random.fold_in(root_key, part))
    shared_keys = jax.random.split(root_key, 16)
    x_in = (0.5 * jax.random.normal(key_x, (BATCH, SEQ_LEN, D_MODEL), jnp.float32)).astype(jnp.bfloat16)
    gain_attn = 1.0 + 0.2 * jax.random.normal(shared_keys[0], (D_MODEL,), jnp.float32)
    gain_mlp = 1.0 + 0.2 * jax.random.normal(shared_keys[1], (D_MODEL,), jnp.float32)
    w_q = draw_normal(shared_keys[2], (D_MODEL, HEADS, HEAD_DIM), 1.7 * D_MODEL ** -0.5)
    w_k = draw_normal(shared_keys[3], (D_MODEL, KV_HEADS, HEAD_DIM), 1.7 * D_MODEL ** -0.5)
    w_v = draw_normal(shared_keys[4], (D_MODEL, KV_HEADS, HEAD_DIM), D_MODEL ** -0.5)
    w_o = draw_normal(shared_keys[5], (HEADS, HEAD_DIM, D_MODEL), Q_WIDTH ** -0.5)
    w_gate = draw_normal(shared_keys[6], (D_MODEL, D_FF), D_MODEL ** -0.5)
    w_up = draw_normal(shared_keys[7], (D_MODEL, D_FF), D_MODEL ** -0.5)
    w_down = draw_normal(shared_keys[8], (D_FF, D_MODEL), D_FF ** -0.5)
    a_q, b_q = lora_pair(shared_keys[9], (ADAPTERS, D_MODEL, RANK), (ADAPTERS, RANK, HEADS, HEAD_DIM), D_MODEL, 1.7)
    a_k, b_k = lora_pair(shared_keys[10], (ADAPTERS, D_MODEL, RANK), (ADAPTERS, RANK, KV_HEADS, HEAD_DIM), D_MODEL, 1.7)
    a_v, b_v = lora_pair(shared_keys[11], (ADAPTERS, D_MODEL, RANK), (ADAPTERS, RANK, KV_HEADS, HEAD_DIM), D_MODEL, 1.0)
    a_o, b_o = lora_pair(shared_keys[12], (ADAPTERS, HEADS, HEAD_DIM, RANK), (ADAPTERS, RANK, D_MODEL), Q_WIDTH, 1.0)
    a_gate, b_gate = lora_pair(shared_keys[13], (ADAPTERS, D_MODEL, RANK), (ADAPTERS, RANK, D_FF), D_MODEL, 1.0)
    a_up, b_up = lora_pair(shared_keys[14], (ADAPTERS, D_MODEL, RANK), (ADAPTERS, RANK, D_FF), D_MODEL, 1.0)
    a_down, b_down = lora_pair(shared_keys[15], (ADAPTERS, D_FF, RANK), (ADAPTERS, RANK, D_MODEL), D_FF, 1.0)
    return dict(x_in=x_in, adapter_ids=draw_ids(key_ids), gain_attn=gain_attn, gain_mlp=gain_mlp,
                w_q=w_q, w_k=w_k, w_v=w_v, w_o=w_o, w_gate=w_gate, w_up=w_up, w_down=w_down,
                a_q=a_q, b_q=b_q, a_k=a_k, b_k=b_k, a_v=a_v, b_v=b_v, a_o=a_o, b_o=b_o,
                a_gate=a_gate, b_gate=b_gate, a_up=a_up, b_up=b_up, a_down=a_down, b_down=b_down)


def rms_scale(x_in, gain_vec):
    x_f32 = x_in.astype(jnp.float32)
    inv_rms = lax.rsqrt(jnp.mean(x_f32 * x_f32, axis=-1, keepdims=True) + RMS_EPS)
    return (x_f32 * inv_rms * gain_vec).astype(jnp.bfloat16)


def lora_proj(h_in, w_base, a_sel, b_sel):
    base_out = jnp.dot(h_in, w_base, preferred_element_type=jnp.float32)
    lora_mid = jnp.dot(h_in, a_sel, preferred_element_type=jnp.float32).astype(jnp.bfloat16)
    return base_out + (LORA_ALPHA / RANK) * jnp.dot(lora_mid, b_sel, preferred_element_type=jnp.float32)


def attend_head(head_item):
    q_head, k_head, v_head = head_item
    scores = jnp.dot(q_head, k_head.T, preferred_element_type=jnp.float32) * HEAD_DIM ** -0.5
    causal = jnp.arange(SEQ_LEN)[:, None] >= jnp.arange(SEQ_LEN)[None, :]
    prob_bf = jax.nn.softmax(jnp.where(causal, scores, -jnp.inf), axis=-1).astype(jnp.bfloat16)
    return jnp.dot(prob_bf, v_head, preferred_element_type=jnp.float32).astype(jnp.bfloat16)


def reference(x_in, adapter_ids, gain_attn, gain_mlp, w_q, w_k, w_v, w_o, w_gate, w_up, w_down,
              a_q, b_q, a_k, b_k, a_v, b_v, a_o, b_o, a_gate, b_gate, a_up, b_up, a_down, b_down):
    head_group = HEADS // KV_HEADS
    w_query = w_q.reshape(D_MODEL, Q_WIDTH)
    w_key = w_k.reshape(D_MODEL, KV_WIDTH)
    w_value = w_v.reshape(D_MODEL, KV_WIDTH)
    w_out = w_o.reshape(Q_WIDTH, D_MODEL)

    def one_sequence(seq_item):
        x_seq, adapter_id = seq_item
        h_norm = rms_scale(x_seq, gain_attn)
        q_all = lora_proj(h_norm, w_query, a_q[adapter_id], b_q[adapter_id].reshape(RANK, Q_WIDTH)).astype(jnp.bfloat16)
        k_all = lora_proj(h_norm, w_key, a_k[adapter_id], b_k[adapter_id].reshape(RANK, KV_WIDTH)).astype(jnp.bfloat16)
        v_all = lora_proj(h_norm, w_value, a_v[adapter_id], b_v[adapter_id].reshape(RANK, KV_WIDTH)).astype(jnp.bfloat16)
        q_heads = q_all.reshape(SEQ_LEN, HEADS, HEAD_DIM).transpose(1, 0, 2)
        k_heads = jnp.repeat(k_all.reshape(SEQ_LEN, KV_HEADS, HEAD_DIM).transpose(1, 0, 2), head_group, axis=0)
        v_heads = jnp.repeat(v_all.reshape(SEQ_LEN, KV_HEADS, HEAD_DIM).transpose(1, 0, 2), head_group, axis=0)
        att_heads = lax.map(attend_head, (q_heads, k_heads, v_heads))
        att_flat = att_heads.transpose(1, 0, 2).reshape(SEQ_LEN, Q_WIDTH)
        z_out = lora_proj(att_flat, w_out, a_o[adapter_id].reshape(Q_WIDTH, RANK), b_o[adapter_id])
        x_one = (x_seq.astype(jnp.float32) + z_out).astype(jnp.bfloat16)
        h_two = rms_scale(x_one, gain_mlp)
        z_gate = lora_proj(h_two, w_gate, a_gate[adapter_id], b_gate[adapter_id]).astype(jnp.bfloat16)
        z_up = lora_proj(h_two, w_up, a_up[adapter_id], b_up[adapter_id]).astype(jnp.bfloat16)
        mlp_mid = (jax.nn.silu(z_gate.astype(jnp.float32)) * z_up.astype(jnp.float32)).astype(jnp.bfloat16)
        z_down = lora_proj(mlp_mid, w_down, a_down[adapter_id], b_down[adapter_id])
        return (x_one.astype(jnp.float32) + z_down).astype(jnp.bfloat16)

    return lax.map(one_sequence, (x_in, adapter_ids))
```

```python
import functools

import jax
import jax.numpy as jnp
from jax import lax
from jax.experimental import pallas as pl
from jax.experimental.pallas import tpu as pltpu
from jax.sharding import PartitionSpec as P

LORA_ALPHA = 16
RMS_EPS = 1e-5
F32 = jnp.float32
BF16 = jnp.bfloat16
VMEM_CAP = 66 * 1000 * 1000
CHUNKS = (8, 8, 8, 4, 4)


def dot_nn(lhs, rhs):
    return lax.dot_general(lhs, rhs, (((1,), (0,)), ((), ())), preferred_element_type=F32)


def dot_nt(lhs, rhs):
    return lax.dot_general(lhs, rhs, (((1,), (1,)), ((), ())), preferred_element_type=F32)


def dot_tn(lhs, rhs):
    return lax.dot_general(lhs, rhs, (((0,), (0,)), ((), ())), preferred_element_type=F32)


def params(dims):
    return pltpu.CompilerParams(dimension_semantics=("arbitrary",) * dims, vmem_limit_bytes=VMEM_CAP)


def cost(flops, nbytes):
    return pl.CostEstimate(flops=int(flops), bytes_accessed=int(nbytes), transcendentals=0)


def keep_own_adapter(mid, ids_ref, first_seq, seq_len, adapter_of_lane):
    parts = []
    for s in range(mid.shape[0] // seq_len):
        rows = mid[s * seq_len:(s + 1) * seq_len]
        parts.append(jnp.where(adapter_of_lane == ids_ref[first_seq + s], rows, 0.0))
    return jnp.concatenate(parts, axis=0).astype(BF16)


def norm_mid_kernel(n_ad, pos_ref, ids_ref, x_ref, gain_ref, a_ref, h_ref, mid_ref, a_scr):
    step = pl.program_id(0)
    groups, rows, _ = a_ref.shape
    n_proj = 3
    per = rows // n_proj

    @pl.when(step == 0)
    def _():
        for g in range(groups):
            for p in range(n_proj):
                a_scr[(p * groups + g) * per:(p * groups + g + 1) * per] = a_ref[g, p * per:(p + 1) * per]

    seqs, seq_len, width = x_ref.shape
    x = x_ref[...].reshape(seqs * seq_len, width).astype(F32)
    inv = lax.rsqrt(jnp.mean(x * x, axis=-1, keepdims=True) + RMS_EPS)
    h = (x * inv * gain_ref[...]).astype(BF16)
    h_ref[...] = h
    mid = dot_nt(h, a_scr[...])
    lane = lax.broadcasted_iota(jnp.int32, (seq_len, mid.shape[1]), 1)
    adapter = (lane // (per // n_ad)) % n_ad
    mid_ref[...] = keep_own_adapter(mid, ids_ref, step * seqs, seq_len, adapter)


def norm_mid(pos, ids, x_in, gain, a_all, n_ad, seqs):
    _, seq_len, width = x_in.shape
    groups, rows, _ = a_all.shape
    bs = 4
    steps = seqs // bs
    tok = bs * seq_len
    grid_spec = pltpu.PrefetchScalarGridSpec(
        num_scalar_prefetch=2, grid=(steps,),
        in_specs=[pl.BlockSpec((bs, seq_len, width), lambda i, pos, ids: (pos[0] * steps + i, 0, 0)),
                  pl.BlockSpec((1, width), lambda i, pos, ids: (0, 0)),
                  pl.BlockSpec((groups, rows, width), lambda i, pos, ids: (0, 0, 0))],
        out_specs=[pl.BlockSpec((tok, width), lambda i, pos, ids: (i, 0)),
                   pl.BlockSpec((tok, groups * rows), lambda i, pos, ids: (i, 0))],
        scratch_shapes=[pltpu.VMEM((groups * rows, width), BF16)])
    total = seqs * seq_len
    return pl.pallas_call(
        functools.partial(norm_mid_kernel, n_ad), grid_spec=grid_spec, name="norm_mid",
        out_shape=[jax.ShapeDtypeStruct((total, width), BF16), jax.ShapeDtypeStruct((total, groups * rows), BF16)],
        compiler_params=params(1), cost_estimate=cost(2 * total * width * groups * rows, 4 * total * width),
    )(pos, ids, x_in, gain, a_all)


def attn_kernel(seq_len, head_dim, scale, h_ref, mq_ref, mk_ref, mv_ref, wq_ref, wk_ref, wv_ref, bq_ref, bk_ref,
                bv_ref, dep_ref, o_ref):
    del dep_ref
    h = h_ref[...]

    def proj(mid_ref, w_ref, b_ref):
        return (dot_nn(h, w_ref[...]) + scale * dot_nn(mid_ref[...], b_ref[...])).astype(BF16)

    q = proj(mq_ref, wq_ref, bq_ref)
    k = proj(mk_ref, wk_ref, bk_ref)
    v = proj(mv_ref, wv_ref, bv_ref)
    row = lax.broadcasted_iota(jnp.int32, (seq_len, seq_len), 0)
    col = lax.broadcasted_iota(jnp.int32, (seq_len, seq_len), 1)
    causal = row >= col
    for s in range(q.shape[0] // seq_len):
        for n in range(q.shape[1] // head_dim):
            rows = slice(s * seq_len, (s + 1) * seq_len)
            cols = slice(n * head_dim, (n + 1) * head_dim)
            sc = dot_nt(q[rows, cols], k[rows, cols]) * head_dim ** -0.5
            sc = jnp.where(causal, sc, -jnp.inf)
            e = jnp.exp(sc - jnp.max(sc, axis=-1, keepdims=True))
            pr = (e / jnp.sum(e, axis=-1, keepdims=True)).astype(BF16)
            o_ref[rows, cols] = dot_nn(pr, v[rows, cols]).astype(BF16)


def attention(h, mid, w3, b3, dep, block, tok, seq_len, head_dim, scale):
    width = h.shape[1]
    cols = w3[0].shape[1]
    tile = 2 * head_dim
    lanes = mid.shape[1] // 3
    w_spec = pl.BlockSpec((width, tile), lambda p: (0, p))
    b_spec = pl.BlockSpec((lanes, tile), lambda p: (0, p))
    mids = [pl.BlockSpec((tok, lanes), functools.partial(lambda j, p: (block, j), j)) for j in range(3)]
    return pl.pallas_call(
        functools.partial(attn_kernel, seq_len, head_dim, scale), grid=(cols // tile,), name="qkv_attn",
        in_specs=[pl.BlockSpec((tok, width), lambda p: (block, 0))] + mids + [w_spec] * 3 + [b_spec] * 3
        + [pl.BlockSpec(memory_space=pl.ANY)],
        out_specs=pl.BlockSpec((tok, tile), lambda p: (0, p)),
        out_shape=jax.ShapeDtypeStruct((tok, cols), BF16),
        compiler_params=params(1), cost_estimate=cost(6 * tok * width * cols * 1.2, 6 * width * cols),
    )(h, mid, mid, mid, *w3, *b3, dep)


def out_kernel(n_ad, scale, pos_ref, ids_ref, x_ref, ao_ref, as_ref, ax_ref, ay_ref, wo_ref, ws_ref, wx_ref, wy_ref,
               lo_ref, b_ref, gain_ref, a_ref, dep_ref, x1_ref, h_ref, mid_ref, mo_scr, a_scr, *, first_seq):
    del dep_ref
    m, n = pl.program_id(0), pl.program_id(1)
    seqs, seq_len, tile = x_ref.shape
    tok = seqs * seq_len
    groups, rows, _ = a_ref.shape
    per = rows // 2
    seq0 = first_seq + m * seqs
    me = pos_ref[2]

    @pl.when((m == 0) & (n == 0))
    def _():
        for g in range(groups):
            for p in range(2):
                a_scr[(p * groups + g) * per:(p * groups + g + 1) * per] = a_ref[g, p * per:(p + 1) * per]

    atts = (ao_ref, as_ref, ax_ref, ay_ref)

    @pl.when(n == 0)
    def _():
        mid = None
        for j, att in enumerate(atts):
            peer = (me + j) % 2 + 2 * ((me // 2 + j // 2) % 2)
            part = dot_nt(att[...], lo_ref[peer])
            mid = part if mid is None else mid + part
        lane = lax.broadcasted_iota(jnp.int32, (seq_len, mid.shape[1]), 1)
        mo_scr[...] = keep_own_adapter(mid, ids_ref, seq0, seq_len, lane // (mid.shape[1] // n_ad))

    z = scale * dot_nn(mo_scr[...], b_ref[0])
    for att, w in zip(atts, (wo_ref, ws_ref, wx_ref, wy_ref)):
        z = z + dot_nn(att[...], w[...])
    x1 = x_ref[...].reshape(tok, tile).astype(F32) + z
    x1_ref[:, pl.ds(pl.multiple_of(n * tile, tile), tile)] = x1.astype(BF16)

    @pl.when(n == pl.num_programs(1) - 1)
    def _():
        v = x1_ref[...].astype(F32)
        inv = lax.rsqrt(jnp.mean(v * v, axis=-1, keepdims=True) + RMS_EPS)
        h = (v * inv * gain_ref[...]).astype(BF16)
        h_ref[...] = h
        mid = dot_nt(h, a_scr[...])
        lane = lax.broadcasted_iota(jnp.int32, (seq_len, mid.shape[1]), 1)
        adapter = (lane // (per // n_ad)) % n_ad
        mid_ref[...] = keep_own_adapter(mid, ids_ref, seq0, seq_len, adapter)


def out_proj(pos, ids, x_in, atts, att_seq, w_os, small, gain, a_all, dep, n_ad, scale, seqs, first_seq, n_seq):
    _, seq_len, width = x_in.shape
    groups, rows, _ = a_all.shape
    bs, tile = 4, 512
    tok = bs * seq_len
    heads = atts[0].shape[1]
    lanes = small.shape[1] // 3
    half = heads // tile
    blk = first_seq // bs
    nb = seqs // bs
    total = n_seq * seq_len
    a_spec = pl.BlockSpec((tok, heads), lambda m, n, pos, ids: (att_seq // bs + m, 0))
    w_spec = pl.BlockSpec((heads, tile), lambda m, n, pos, ids: (0, n))
    full = lambda m, n, pos, ids: (m, 0)
    grid_spec = pltpu.PrefetchScalarGridSpec(
        num_scalar_prefetch=2, grid=(n_seq // bs, width // tile),
        in_specs=[pl.BlockSpec((bs, seq_len, tile), lambda m, n, pos, ids: (pos[0] * nb + blk + m, 0, n))]
        + [a_spec] * 4 + [w_spec] * 4
        + [pl.BlockSpec((4, lanes, heads), lambda m, n, pos, ids: (0, 0, 0)),
           pl.BlockSpec((1, lanes, tile), lambda m, n, pos, ids: (n // half, 1, n % half)),
           pl.BlockSpec((1, width), lambda m, n, pos, ids: (0, 0)),
           pl.BlockSpec((groups, rows, width), lambda m, n, pos, ids: (0, 0, 0)),
           pl.BlockSpec(memory_space=pl.ANY)],
        out_specs=[pl.BlockSpec((tok, width), full), pl.BlockSpec((tok, width), full),
                   pl.BlockSpec((tok, groups * rows), full)],
        scratch_shapes=[pltpu.VMEM((tok, lanes), BF16), pltpu.VMEM((groups * rows, width), BF16)])
    return pl.pallas_call(
        functools.partial(out_kernel, n_ad, scale, first_seq=first_seq), grid_spec=grid_spec, name="out_proj",
        out_shape=[jax.ShapeDtypeStruct((total, width), BF16), jax.ShapeDtypeStruct((total, width), BF16),
                   jax.ShapeDtypeStruct((total, groups * rows), BF16)],
        compiler_params=params(2), cost_estimate=cost(2 * total * width * (width + 512), 8 * total * width),
    )(pos, ids, x_in, *atts, *w_os, small, small, gain, a_all, dep)


def mlp_kernel(n_ad, scale, up_steps, pos_ref, h_ref, mg_ref, mu_ref, g0_ref, g1_ref, u0_ref, u1_ref, bg0_ref, bg1_ref,
               bu0_ref, bu1_ref, d0_ref, d1_ref, l0_ref, l1_ref, tok_ref, ss_ref, sk_ref, ms_ref, mk_ref, m0_scr,
               m1_scr):
    i = pl.program_id(0)
    cols = d0_ref.shape[0]
    tile = g0_ref.shape[0]
    half = ss_ref.shape[0]
    chip = pos_ref[1]

    @pl.when(i < up_steps)
    def _():
        h = h_ref[...]
        at = pl.ds(pl.multiple_of(i * tile, tile), tile)
        for g_ref, u_ref, bg_ref, bu_ref, m_scr in ((g0_ref, u0_ref, bg0_ref, bu0_ref, m0_scr),
                                                    (g1_ref, u1_ref, bg1_ref, bu1_ref, m1_scr)):
            gate = (dot_nt(h, g_ref[...]) + scale * dot_nn(mg_ref[...], bg_ref[...])).astype(BF16).astype(F32)
            up = (dot_nt(h, u_ref[...]) + scale * dot_nn(mu_ref[...], bu_ref[...])).astype(BF16).astype(F32)
            m_scr[:, at] = (jax.nn.silu(gate) * up).astype(BF16)

    send_rows = pl.ds(pl.multiple_of((1 - chip) * half, half), half)
    keep_rows = pl.ds(pl.multiple_of(chip * half, half), half)

    @pl.when(i == up_steps)
    def _():
        for rows, out in ((send_rows, ms_ref), (keep_rows, mk_ref)):
            mid = dot_nt(l0_ref[...], m0_scr[rows, :cols]) + dot_nt(l1_ref[...], m1_scr[rows, :cols])
            lanes = mid.shape[0]
            row = lax.broadcasted_iota(jnp.int32, mid.shape, 0)
            ids = jnp.where(rows is send_rows, tok_ref[0:1, :], tok_ref[1:2, :])
            mid = jnp.where(row // (lanes // n_ad) == ids, mid, 0.0)
            out[...] = jnp.sum(mid.reshape(n_ad, lanes // n_ad, half), axis=0)

    @pl.when(i >= up_steps)
    def _():
        for rows, out in ((send_rows, ss_ref), (keep_rows, sk_ref)):
            part = dot_nn(m0_scr[rows, :cols], d0_ref[...]) + dot_nn(m1_scr[rows, :cols], d1_ref[...])
            out[...] = part.astype(BF16)


def mlp(pos, h2, mid, gates, ups, b_gates, b_ups, downs, a_downs, tok_ids, n_ad, scale):
    tok, width = h2.shape
    cols = gates[0].shape[0]
    tile, dtile = 256, 512
    up_steps = pl.cdiv(cols, tile)
    down_steps = width // dtile
    lanes = mid.shape[1] // 2
    half = tok // 2
    rank = a_downs[0].shape[0] // n_ad
    const = lambda i, pos: (0, 0)
    g_spec = pl.BlockSpec((tile, width), lambda i, pos: (jnp.minimum(i, up_steps - 1), 0))
    b_spec = pl.BlockSpec((lanes, tile), lambda i, pos: (0, jnp.minimum(i, up_steps - 1)))
    d_spec = pl.BlockSpec((cols, dtile), lambda i, pos: (0, jnp.maximum(i - up_steps, 0)))
    s_spec = pl.BlockSpec((half, dtile), lambda i, pos: (0, jnp.maximum(i - up_steps, 0)))
    grid_spec = pltpu.PrefetchScalarGridSpec(
        num_scalar_prefetch=1, grid=(up_steps + down_steps,),
        in_specs=[pl.BlockSpec((tok, width), const, pipeline_mode=pl.Buffered(1)),
                  pl.BlockSpec((tok, lanes), lambda i, pos: (0, 0)),
                  pl.BlockSpec((tok, lanes), lambda i, pos: (0, 1))]
        + [g_spec] * 4 + [b_spec] * 4 + [d_spec] * 2
        + [pl.BlockSpec((n_ad * rank, cols), const)] * 2 + [pl.BlockSpec((2, half), const)],
        out_specs=[s_spec, s_spec, pl.BlockSpec((rank, half), const), pl.BlockSpec((rank, half), const)],
        scratch_shapes=[pltpu.VMEM((tok, up_steps * tile), BF16)] * 2)
    return pl.pallas_call(
        functools.partial(mlp_kernel, n_ad, scale, up_steps), grid_spec=grid_spec, name="mlp",
        out_shape=[jax.ShapeDtypeStruct((half, width), BF16)] * 2 + [jax.ShapeDtypeStruct((rank, half), F32)] * 2,
        compiler_params=params(1), cost_estimate=cost(12 * tok * width * cols, 12 * width * cols),
    )(pos, h2, mid, mid, *gates, *ups, *b_gates, *b_ups, *downs, *a_downs, tok_ids)


def final_kernel(n_ad, scale, pos_ref, x1_ref, sk_ref, sr_ref, mk_ref, mr_ref, b_ref, tok_ref, dep_ref, y_ref):
    del dep_ref
    mid = (mk_ref[...] + mr_ref[...]).astype(BF16).astype(F32)
    rank, tok = mid.shape
    wide = jnp.concatenate([mid] * n_ad, axis=0)
    row = lax.broadcasted_iota(jnp.int32, wide.shape, 0)
    wide = jnp.where(row // rank == tok_ref[1:2, :], wide, 0.0).astype(BF16)
    cols = b_ref.shape[2]
    for g in range(b_ref.shape[0]):
        at = slice(g * cols, (g + 1) * cols)
        part = sk_ref[:, at].astype(F32) + sr_ref[:, at].astype(F32)
        y = x1_ref[:, at].astype(F32) + part + scale * dot_tn(wide, b_ref[g])
        y_ref[:, at] = y.astype(BF16)


def final_sum(pos, x1, s_keep, s_recv, m_keep, m_recv, small, tok_ids, dep, n_ad, scale):
    half, width = s_keep.shape
    rank = m_keep.shape[0]
    lanes, cols = small.shape[1] // 3, small.shape[2]
    rows = 256
    steps = half // rows
    row_spec = pl.BlockSpec((rows, width), lambda i, pos: (i, 0))
    mid_spec = pl.BlockSpec((rank, rows), lambda i, pos: (0, i))
    grid_spec = pltpu.PrefetchScalarGridSpec(
        num_scalar_prefetch=1, grid=(steps,),
        in_specs=[pl.BlockSpec((rows, width), lambda i, pos: (pos[1] * steps + i, 0)), row_spec, row_spec,
                  mid_spec, mid_spec, pl.BlockSpec((4, lanes, cols), lambda i, pos: (0, 2, 0)),
                  pl.BlockSpec((2, rows), lambda i, pos: (0, i)), pl.BlockSpec(memory_space=pl.ANY)],
        out_specs=row_spec)
    return pl.pallas_call(
        functools.partial(final_kernel, n_ad, scale), grid_spec=grid_spec, name="final_sum",
        out_shape=jax.ShapeDtypeStruct((half, width), BF16),
        compiler_params=params(1), cost_estimate=cost(2 * half * width * lanes, 8 * half * width),
    )(pos, x1, s_keep, s_recv, m_keep, m_recv, small, tok_ids, dep)


def solution(mesh):
    act_spec = P('dp', None, None)
    w_head_spec = P(None, 'tp', None)
    w_out_spec = P('tp', None, None)
    w_col_spec = P(None, 'tp')
    w_row_spec = P('tp', None)
    a_rank_spec = P(None, None, 'tp')
    b_head_spec = P(None, None, 'tp', None)
    b_col_spec = P(None, None, 'tp')
    a_head_spec = P(None, 'tp', None, None)
    a_row_spec = P(None, 'tp', None)
    in_specs = (act_spec, P('dp'), P(None), P(None), w_head_spec, w_head_spec, w_head_spec, w_out_spec,
                w_col_spec, w_col_spec, w_row_spec, a_rank_spec, b_head_spec, a_rank_spec, b_head_spec,
                a_rank_spec, b_head_spec, a_head_spec, b_col_spec, a_rank_spec, b_col_spec,
                a_rank_spec, b_col_spec, a_row_spec, b_col_spec)

    def to_core(v):
        return lax.ppermute(v, 'tp', [(0, 1), (1, 0), (2, 3), (3, 2)])

    def to_chip(v):
        return lax.ppermute(v, 'tp', [(0, 2), (2, 0), (1, 3), (3, 1)])

    def to_row(v):
        return lax.ppermute(v, 'dp', [(0, 1), (1, 0)])

    def after(v, dep):
        return lax.optimization_barrier((v, dep))[0]

    def local_layer(x_in, adapter_ids, gain_attn, gain_mlp, w_q, w_k, w_v, w_o, w_gate, w_up, w_down,
                    a_q, b_q, a_k, b_k, a_v, b_v, a_o, b_o, a_gate, b_gate, a_up, b_up, a_down, b_down):
        n_seq, seq_len, width = x_in.shape
        head_dim = w_q.shape[2]
        n_ad, rank = b_q.shape[0], b_q.shape[1]
        scale = LORA_ALPHA / rank
        rank_loc = a_q.shape[2]
        tp = rank // rank_loc
        seqs = n_seq // 2
        me = lax.axis_index('tp')
        row = lax.axis_index('dp')
        core, chip = me % 2, me // 2
        pos = jnp.stack([core, chip, me]).astype(jnp.int32)
        ids = lax.dynamic_slice_in_dim(adapter_ids, core * seqs, seqs)

        wo = w_o.reshape(-1, width)
        n_half = wo.shape[0] // 2
        wo_half = to_chip(lax.dynamic_slice_in_dim(wo, row * n_half, n_half, 0))

        def rank_rows(a):
            return a.transpose(0, 2, 1).reshape(n_ad * rank_loc, width)

        a_qkv = lax.all_gather(jnp.concatenate([rank_rows(a) for a in (a_q, a_k, a_v)]), 'tp')
        a_gu = lax.all_gather(jnp.concatenate([rank_rows(a) for a in (a_gate, a_up)]), 'tp')
        a_o2 = a_o.transpose(0, 3, 1, 2).reshape(n_ad * rank, -1)
        small = jnp.concatenate([a_o2, b_o.reshape(n_ad * rank, -1), b_down.reshape(n_ad * rank, -1)])
        small = lax.all_gather(small, 'tp')

        def by_device(b):
            cols = b.reshape(n_ad, tp, rank_loc, -1)
            return cols.transpose(1, 0, 2, 3).reshape(n_ad * rank, -1)

        w3 = [w.reshape(width, -1) for w in (w_q, w_k, w_v)]
        b3 = [by_device(b) for b in (b_q, b_k, b_v)]
        w3_sib, b3_sib = [to_core(w) for w in w3], [to_core(b) for b in b3]
        gates = (w_gate.T, to_core(w_gate.T))
        ups = (w_up.T, to_core(w_up.T))
        downs = (w_down, to_core(w_down))
        bg, bu = by_device(b_gate), by_device(b_up)
        b_gates, b_ups = (bg, to_core(bg)), (bu, to_core(bu))
        a_dn = a_down.transpose(0, 2, 1).reshape(n_ad * rank, -1)
        a_downs = (a_dn, to_core(a_dn))

        h, mid = norm_mid(pos, ids, x_in, gain_attn.reshape(1, -1), a_qkv, n_ad, seqs)

        blk = 8
        tok = blk * seq_len
        att = {}
        dep = ids
        for name, w, b in (('own', w3, b3), ('sib', w3_sib, b3_sib)):
            att[name] = []
            for j in range(seqs // blk):
                out = attention(h, mid, w, b, dep, j, tok, seq_len, head_dim, scale)
                att[name].append(out)
                dep = out
        att_x = [to_chip(a) for a in att['own']]
        att_y = [to_chip(a) for a in att['sib']]

        wo_half = after(wo_half, h)
        wo_rest = after(to_row(wo_half), att['own'][2])
        wo_x = jnp.where(row == 0, jnp.concatenate([wo_half, wo_rest]), jnp.concatenate([wo_rest, wo_half]))
        w_os = (wo, to_core(wo), wo_x, to_core(wo_x))

        y = jnp.zeros((n_seq, seq_len, width), BF16)
        done, late = [], []

        def finish(args, dep):
            first, sub, x1, s_keep, s_recv, m_keep, m_recv, tok_ids = args
            y_own = final_sum(pos, x1, s_keep, s_recv, m_keep, m_recv, small, tok_ids, dep, n_ad, scale)
            y_own = y_own.reshape(sub, seq_len, width)
            y_x = to_chip(y_own)
            return first, sub, y_own, y_x

        def place(y, args, dep):
            first, sub, y_own, y_x = args
            y_s, y_y = to_core(y_own), to_core(y_x)
            parts = ((y_own, core, chip), (y_x, core, 1 - chip), (y_s, 1 - core, chip), (y_y, 1 - core, 1 - chip))
            for part, c, k in parts:
                y = lax.dynamic_update_slice_in_dim(y, after(part, dep), c * seqs + first + k * sub, 0)
            return y

        first = 0
        for size in CHUNKS:
            j = first // blk
            atts = [a[j] for a in (att['own'], att['sib'], att_x, att_y)]
            x1, h2, mid2 = out_proj(pos, ids, x_in, atts, first % blk, w_os, small, gain_mlp.reshape(1, -1), a_gu,
                                    dep, n_ad, scale, seqs, first, size)
            sub = size // 2
            seq_send = lax.dynamic_slice_in_dim(ids, first + (1 - chip) * sub, sub)
            seq_keep = lax.dynamic_slice_in_dim(ids, first + chip * sub, sub)
            tok_ids = jnp.repeat(jnp.stack([seq_send, seq_keep]), seq_len, axis=1)
            s_send, s_keep, m_send, m_keep = mlp(pos, h2, mid2, gates, ups, b_gates, b_ups, downs, a_downs, tok_ids,
                                                 n_ad, scale)
            dep = m_send
            if late:
                y = place(y, late.pop(0), dep)
            if done:
                late.append(finish(done.pop(0), dep))
                dep = late[-1][2]
            done.append((first, sub, x1, s_keep, to_chip(s_send), m_keep, to_chip(m_send), tok_ids))
            first += size
        late.append(finish(done.pop(0), dep))
        for args in late:
            y = place(y, args, dep)
        return y

    return jax.shard_map(local_layer, mesh=mesh, in_specs=in_specs, out_specs=act_spec, check_vma=False)
```
